32 devices in a mesh: dp: 4 (over x, core), vocab: 8 (over z, y).
Axes of the slice: x: 2, y: 2, z: 4, core: 2. Of those that a mesh axis runs over, the one named last changes fastest.
Arguments:
- policy_hidden: bfloat16 [512, 4096], P('dp'), may hold values from -84 to 84
- policy_weight: bfloat16 [4096, 65536], P('dp', 'vocab'), may hold values from -0.09375 to 0.09375
- reference_hidden: bfloat16 [512, 4096], P(('dp', 'vocab')), may hold values from -84 to 84
- reference_weight: bfloat16 [4096, 65536], P(None, ('dp', 'vocab')), may hold values from -0.09375 to 0.09375
- targets: int32 [512], replicated, may hold values from 0 to 65535
- response_mask: int32 [512], replicated, may hold values 0 or 1
- pair_index: int32 [16], replicated, may hold values from 0 to 15, each once
Outputs:
- hidden_grad: bfloat16 [512, 4096], P('vocab', 'dp')
- weight_grad: bfloat16 [4096, 65536], P('dp', 'vocab')
- total_loss: float32 [], replicated
The draws below stay inside these ranges and needn't reach their ends.
Inputs may be any that keep to these rules, and one draw needn't show every extreme that they name: `pair_index`: each number of 0 to 15 once; entries 2p and 2p + 1 are the chosen and the rejected sequence of pair p.
All inputs are finite; a program needn't handle non-finite values.
Results may differ from the reference program's by a relative error of at most 0.005.
The reference program's roundings to bfloat16 on the way (of `logit_grad`) count: a program that leaves them out, or rounds other values in their place, can miss the bound.
Values may be sent and summed in bfloat16 or wider, within the bound.
A program may use at most 128 MiB of HBM per device.

```python
import math
import jax
import jax.numpy as jnp
import numpy as np
from jax import lax

D = 4096
VOCAB = 65536
SEQ_LEN = 32
SEQS = 16
TOKENS = 512


def scaled_rows(key, salt):
    folded = jax.random.fold_in(key, salt)
    key_value = jax.random.fold_in(folded, 1)
    return 3.0 * jnp.clip(jax.random.normal(key_value, (TOKENS, D), jnp.float32), -6.0, 6.0)


def draw_policy_hidden(key, part):
    return scaled_rows(key, 11).astype(jnp.bfloat16)


def draw_reference_hidden(key, part):
    return scaled_rows(key, 23).astype(jnp.bfloat16)


def touch_ends(array, stream_key, smallest, top_value):
    longest = array.shape.index(max(array.shape))
    spots = []
    for shift in (0, 1):
        where = [jax.random.randint(jax.random.fold_in(stream_key, axis), (), 0, length) for axis, length in enumerate(array.shape)]
        where[longest] = (where[longest] + shift) % array.shape[longest]
        spots.append(tuple(where))
    return array.at[spots[0]].set(smallest).at[spots[1]].set(top_value)


def levels(stream_key, shape, cuts, least, high):
    def one(axis_at, parts):
        steps = jax.random.uniform(jax.random.fold_in(jax.random.fold_in(stream_key, 6), axis_at), (parts,), jnp.float32, least / len(cuts), high / len(cuts))
        return jnp.repeat(jnp.exp(steps), shape[axis_at] // parts).reshape((-1,) + (1,) * (len(shape) - axis_at - 1))

    level = one(*cuts[0])
    for cut in cuts[1:]:
        level = level * one(*cut)
    return level


def rank_bounds(amount, skew):
    weights = [(1 << 20) // math.isqrt(standing ** skew) + 1 for standing in range(1, amount + 1)]
    scale = 1 + sum(weights) // (1 << 30)
    return np.cumsum(np.array([max(1, weight // scale) for weight in weights]))


def skewed_ids(stream_key, dims, amount, slope):
    listing = rank_bounds(amount, slope)
    lot = jax.random.randint(jax.random.fold_in(stream_key, 1), dims, 0, int(listing[amount - 1]))
    standing = jnp.searchsorted(jnp.asarray(listing, jnp.int32), lot, side="right")
    return jax.random.permutation(jax.random.fold_in(stream_key, 2), amount)[standing].astype(jnp.int32)


def scatter_about(key, dims, scale, reach, shards=(), kind=jnp.bfloat16):
    array = jax.random.normal(key, dims, jnp.float32) * scale
    if len(shards) > 0:
        array = levels(key, dims, shards, -0.22, 0.18) * array
    return jnp.clip(array, min=-reach, max=reach).astype(kind)


def setup_inputs(seed: int = 0) -> dict:
    key_of = jax.random.split(jax.random.key(seed), 8)
    policy_hidden = draw_policy_hidden(jax.random.fold_in(key_of[7], 71), 0)
    policy_weight = scatter_about(key_of[1], (D, VOCAB), D ** -0.5, 0.09375, ((0, 4), (1, 8)))
    reference_hidden = draw_reference_hidden(jax.random.fold_in(key_of[7], 71), 0)
    reference_weight = scatter_about(key_of[3], (D, VOCAB), D ** -0.5, 0.09375, ((1, 32),))
    targets = touch_ends(skewed_ids(key_of[4], (TOKENS,), VOCAB, 2), jax.random.fold_in(key_of[4], 3), 0, VOCAB - 1).astype(jnp.int32)
    response_mask = touch_ends((jax.random.randint(key_of[5], (TOKENS,), 0, 4) < 3).astype(jnp.int32), jax.random.fold_in(key_of[5], 1), 0, 1)
    pair_index = jax.random.permutation(key_of[6], SEQS).astype(jnp.int32)
    return {"policy_hidden": policy_hidden, "policy_weight": policy_weight, "reference_hidden": reference_hidden, "reference_weight": reference_weight, "targets": targets, "response_mask": response_mask, "pair_index": pair_index}


beta = 0.1
loss_scale = 4096.0
block_size = 64


def pair_terms(log_ratio, pair_index):
    chosen = pair_index[0::2]
    rejected = pair_index[1::2]
    margin = beta * (log_ratio[chosen] - log_ratio[rejected])
    pair_count = chosen.shape[0]
    total_loss = jnp.sum(jax.nn.softplus(-margin)) / pair_count
    weight = -beta * loss_scale * jax.nn.sigmoid(-margin) / pair_count
    numbers = jnp.arange(log_ratio.shape[0], dtype=jnp.int32)[:, None]
    factor = jnp.sum(jnp.where(numbers == chosen[None, :], weight[None, :], 0.0) - jnp.where(numbers == rejected[None, :], weight[None, :], 0.0), axis=1)
    return total_loss, factor


def token_logp(hidden, weight, targets):
    blocks = hidden.shape[0] // block_size

    def block_logp(inputs):
        row_block, target_block = inputs
        logits = jnp.dot(row_block, weight, preferred_element_type=jnp.float32)
        largest = jnp.max(logits, axis=1)
        exp_total = jnp.sum(jnp.exp(logits - largest[:, None]), axis=1)
        picked = jnp.take_along_axis(logits, target_block[:, None], axis=1)[:, 0]
        return picked - largest - jnp.log(exp_total)

    return lax.map(block_logp, (hidden.reshape(blocks, block_size, hidden.shape[1]), targets.reshape(blocks, block_size))).reshape(-1)


def reference(policy_hidden, policy_weight, reference_hidden, reference_weight, targets, response_mask, pair_index):
    policy_logp = token_logp(policy_hidden, policy_weight, targets)
    reference_logp = token_logp(reference_hidden, reference_weight, targets)
    active = response_mask.astype(jnp.float32)
    log_ratio = jnp.sum((active * (policy_logp - reference_logp)).reshape(-1, SEQ_LEN), axis=1)
    total_loss, factor = pair_terms(log_ratio, pair_index)
    token_scale = active * jnp.repeat(factor, SEQ_LEN)
    blocks = policy_hidden.shape[0] // block_size
    vocab_ids = lax.broadcasted_iota(jnp.int32, (block_size, policy_weight.shape[1]), 1)

    def backward(weight_grad, inputs):
        row_block, target_block, scale_block = inputs
        logits = jnp.dot(row_block, policy_weight, preferred_element_type=jnp.float32)
        largest = jnp.max(logits, axis=1, keepdims=True)
        log_total = largest + jnp.log(jnp.sum(jnp.exp(logits - largest), axis=1, keepdims=True))
        onehot = (vocab_ids == target_block[:, None]).astype(jnp.float32)
        logit_grad = (scale_block[:, None] * (onehot - jnp.exp(logits - log_total))).astype(jnp.bfloat16)
        weight_grad = weight_grad + jnp.dot(row_block.T, logit_grad, preferred_element_type=jnp.float32)
        row_grad = jnp.dot(logit_grad, policy_weight.T, preferred_element_type=jnp.float32).astype(jnp.bfloat16)
        return weight_grad, row_grad

    weight_grad, hidden_grad = lax.scan(backward, jnp.zeros(policy_weight.shape, jnp.float32), (policy_hidden.reshape(blocks, block_size, policy_hidden.shape[1]), targets.reshape(blocks, block_size), token_scale.reshape(blocks, block_size)))
    return hidden_grad.reshape(policy_hidden.shape), weight_grad.astype(jnp.bfloat16), total_loss
```

```python
import functools

import jax
import jax.numpy as jnp
from jax import lax
from jax.experimental import pallas as pl
from jax.experimental.pallas import tpu as pltpu
from jax.sharding import PartitionSpec as P

SEQ_LEN = 32


beta = 0.1
loss_scale = 4096.0


def pair_terms(log_ratio, pair_index):
    chosen = pair_index[0::2]
    rejected = pair_index[1::2]
    margin = beta * (log_ratio[chosen] - log_ratio[rejected])
    pair_count = chosen.shape[0]
    total_loss = jnp.sum(jax.nn.softplus(-margin)) / pair_count
    weight = -beta * loss_scale * jax.nn.sigmoid(-margin) / pair_count
    numbers = jnp.arange(log_ratio.shape[0], dtype=jnp.int32)[:, None]
    factor = jnp.sum(
        jnp.where(numbers == chosen[None, :], weight[None, :], 0.0)
        - jnp.where(numbers == rejected[None, :], weight[None, :], 0.0),
        axis=1,
    )
    return (total_loss, factor)


def local_pick(logits, targets, offset, axis):
    column_ids = lax.broadcasted_iota(jnp.int32, logits.shape, axis)
    shifted = targets - offset
    wanted = shifted[:, None]
    return jnp.sum(jnp.where(column_ids == wanted, logits, 0.0), axis=axis)


def gather_kernel(nd, nv, x_ref, out_ref, own_sem, send_d, recv_d, send_v, recv_v):
    d, v = lax.axis_index("dp"), lax.axis_index("vocab")
    data_peers = [lax.rem(d + k, nd) for k in range(1, nd)]
    vocab_peers = [lax.rem(v + k, nv) for k in range(1, nv)]
    barrier = pltpu.get_barrier_semaphore()
    for peer in data_peers:
        pl.semaphore_signal(
            barrier, inc=1, device_id=(peer, v), device_id_type=pl.DeviceIdType.MESH
        )
    for peer in vocab_peers:
        pl.semaphore_signal(
            barrier, inc=1, device_id=(d, peer), device_id_type=pl.DeviceIdType.MESH
        )
    pl.semaphore_wait(barrier, nd + nv - 2)
    own = pltpu.make_async_copy(x_ref, out_ref.at[v, d], own_sem)
    own.start()
    copies = [
        pltpu.make_async_remote_copy(
            src_ref=x_ref,
            dst_ref=out_ref.at[v, d],
            send_sem=send_d.at[k],
            recv_sem=recv_d.at[k],
            device_id=(peer, v),
            device_id_type=pl.DeviceIdType.MESH,
        )
        for k, peer in enumerate(data_peers)
    ]
    for copy in copies:
        copy.start()
    own.wait()
    for copy in copies:
        copy.wait()
    copies = [
        pltpu.make_async_remote_copy(
            src_ref=out_ref.at[v],
            dst_ref=out_ref.at[v],
            send_sem=send_v.at[k],
            recv_sem=recv_v.at[k],
            device_id=(d, peer),
            device_id_type=pl.DeviceIdType.MESH,
        )
        for k, peer in enumerate(vocab_peers)
    ]
    for copy in copies:
        copy.start()
    for copy in copies:
        copy.wait()


def gather_stats(stats):
    nd, nv = lax.axis_size("dp"), lax.axis_size("vocab")
    size = stats.shape[0]
    rows = -(-size // 1024) * 8
    stats = jnp.pad(stats, (0, rows * 128 - size)).reshape(rows, 128)
    gathered = pl.pallas_call(
        functools.partial(gather_kernel, nd, nv),
        out_shape=jax.ShapeDtypeStruct((nv, nd, rows, 128), jnp.float32),
        in_specs=[pl.BlockSpec(memory_space=pltpu.VMEM)],
        out_specs=pl.BlockSpec(memory_space=pltpu.VMEM),
        scratch_shapes=[
            pltpu.SemaphoreType.DMA,
            pltpu.SemaphoreType.DMA((nd - 1,)),
            pltpu.SemaphoreType.DMA((nd - 1,)),
            pltpu.SemaphoreType.DMA((nv - 1,)),
            pltpu.SemaphoreType.DMA((nv - 1,)),
        ],
        compiler_params=pltpu.CompilerParams(collective_id=0, has_side_effects=True),
        name="gather_stats",
    )(stats)
    return gathered.reshape(nv, nd, rows * 128)[:, :, :size]


def grad_kernel(rows_ref, segment_ref, out_ref):
    out_ref[...] = jnp.dot(
        rows_ref[...], segment_ref[...], preferred_element_type=jnp.float32
    ).astype(out_ref.dtype)


def grad_matmul(rows, segment):
    depth, tokens = rows.shape
    width = segment.shape[1]
    tile = 512 if width % 512 == 0 else width
    return pl.pallas_call(
        grad_kernel,
        grid=(width // tile,),
        in_specs=[
            pl.BlockSpec((depth, tokens), lambda i: (0, 0)),
            pl.BlockSpec((tokens, tile), lambda i: (0, i)),
        ],
        out_specs=pl.BlockSpec((depth, tile), lambda i: (0, i)),
        out_shape=jax.ShapeDtypeStruct((depth, width), jnp.bfloat16),
        cost_estimate=pl.CostEstimate(
            flops=2 * depth * tokens * width,
            bytes_accessed=2 * (depth * tokens + tokens * width + depth * width),
            transcendentals=0,
        ),
        name="weight_grad",
    )(rows, segment)


def local(
    policy_hidden,
    policy_weight,
    reference_hidden,
    reference_weight,
    targets,
    response_mask,
    pair_index,
):
    data_index = lax.axis_index("dp")
    vocab_index = lax.axis_index("vocab")
    vocab_devices = lax.axis_size("vocab")
    local_tokens = policy_hidden.shape[0]
    policy_width = policy_weight.shape[1]
    reference_width = reference_weight.shape[1]
    active = response_mask.astype(jnp.float32)
    columns = lax.all_to_all(policy_hidden, "dp", split_axis=1, concat_axis=0, tiled=True)
    reference_logits = jnp.dot(
        lax.all_gather(reference_hidden, ("dp", "vocab"), axis=0, tiled=True),
        reference_weight,
        preferred_element_type=jnp.float32,
    )
    reference_offset = (data_index * vocab_devices + vocab_index) * reference_width
    reference_top = jnp.max(reference_logits, axis=1)
    reference_sum = jnp.sum(jnp.exp(reference_logits - reference_top[:, None]), axis=1)
    reference_pick = local_pick(reference_logits, targets, reference_offset, 1)
    policy_logits = lax.psum_scatter(
        jnp.dot(columns, policy_weight, preferred_element_type=jnp.float32),
        "dp",
        scatter_dimension=0,
        tiled=True,
    )
    own_targets = lax.dynamic_slice_in_dim(targets, data_index * local_tokens, local_tokens, 0)
    policy_offset = vocab_index * policy_width
    policy_pick = local_pick(policy_logits, own_targets, policy_offset, 1)
    policy_top = jnp.max(policy_logits, axis=1)
    policy_sum = jnp.sum(jnp.exp(policy_logits - policy_top[:, None]), axis=1)
    stats = jnp.concatenate(
        [policy_top, policy_sum, policy_pick, reference_top, reference_sum, reference_pick]
    )
    stats = gather_stats(stats)
    tokens = targets.shape[0]
    policy_stats = stats[:, :, : 3 * local_tokens].reshape(vocab_devices, -1, 3, local_tokens)
    policy_max = jnp.max(policy_stats[:, :, 0], axis=0)
    policy_scaled = policy_stats[:, :, 1] * jnp.exp(policy_stats[:, :, 0] - policy_max[None])
    policy_totals = (policy_max + jnp.log(jnp.sum(policy_scaled, axis=0))).reshape(tokens)
    policy_logp = jnp.sum(policy_stats[:, :, 2], axis=0).reshape(tokens) - policy_totals
    reference_stats = stats[:, :, 3 * local_tokens :].reshape(-1, 3, tokens)
    reference_max = jnp.max(reference_stats[:, 0], axis=0)
    reference_scaled = reference_stats[:, 1] * jnp.exp(reference_stats[:, 0] - reference_max[None])
    reference_logp = (
        jnp.sum(reference_stats[:, 2], axis=0)
        - reference_max
        - jnp.log(jnp.sum(reference_scaled, axis=0))
    )
    log_ratio = jnp.sum((active * (policy_logp - reference_logp)).reshape(-1, SEQ_LEN), axis=1)
    total_loss, factor = pair_terms(log_ratio, pair_index)
    token_scale = lax.dynamic_slice_in_dim(
        active * jnp.repeat(factor, SEQ_LEN), data_index * local_tokens, local_tokens, 0
    )
    policy_total = lax.dynamic_slice_in_dim(
        policy_totals, data_index * local_tokens, local_tokens, 0
    )
    column_ids = lax.broadcasted_iota(jnp.int32, policy_logits.shape, 1)
    onehot = (column_ids == (own_targets - policy_offset)[:, None]).astype(jnp.float32)
    logit_grad = (
        token_scale[:, None] * (onehot - jnp.exp(policy_logits - policy_total[:, None]))
    ).astype(jnp.bfloat16)
    segment = lax.all_gather(logit_grad, "dp", axis=0, tiled=True)
    hidden_piece = lax.dot_general(
        segment, policy_weight, (((1,), (1,)), ((), ())), preferred_element_type=jnp.float32
    )
    pieces = lax.all_to_all(
        hidden_piece.astype(jnp.bfloat16).reshape(vocab_devices, -1, hidden_piece.shape[1]),
        "vocab",
        split_axis=0,
        concat_axis=0,
    )
    hidden_grad = jnp.sum(pieces.astype(jnp.float32), axis=0)
    weight_grad = grad_matmul(columns.T, segment)
    return (hidden_grad.astype(jnp.bfloat16), weight_grad, total_loss)


def solution(mesh):
    placed = (
        P("dp", None),
        P("dp", "vocab"),
        P(("dp", "vocab"), None),
        P(None, ("dp", "vocab")),
        P(),
        P(),
        P(),
    )
    return jax.shard_map(
        local,
        mesh=mesh,
        in_specs=placed,
        out_specs=(P("vocab", "dp"), P("dp", "vocab"), P()),
        check_vma=False,
    )
```
